32 devices in a mesh: expert: 8 (over z, x), pair: 4 (over y, core).
Axes of the slice: x: 2, y: 2, z: 4, core: 2. Of those that a mesh axis runs over, the one named last changes fastest.
Arguments:
- tokens: bfloat16 [12288, 2048], P(('expert', 'pair')), may hold values from -6 to 6
- token_ids: int32 [12288], P(('expert', 'pair')), may hold values from 0 to 8191
- table: int32 [8192], replicated, may hold values from 0 to 15
- w_in: bfloat16 [16, 2048, 2048], P('expert', None, 'pair'), may hold values from -0.125 to 0.125
- w_out: bfloat16 [16, 2048, 2048], P('expert', 'pair'), may hold values from -0.125 to 0.125
Outputs:
- mixed: bfloat16 [12288, 2048], P(('expert', 'pair'))
The draws below stay inside these ranges and needn't reach their ends.
All inputs are finite; a program needn't handle non-finite values.
Results may differ from the reference program's by a relative error of at most 0.0085.
Values may be sent and summed in bfloat16 or wider, within the bound.
A program may use at most 192 MiB of HBM per device.

```python
import math
import jax
import jax.numpy as jnp
import numpy as np
from jax import lax

D = 2048
H = 2048
VOCAB = 8192
TOK_DEV = 384
EXPERTS = 16
CAP = 48
TOKENS = 12288
N_EXPERT = 8
N_PAIR = 4


def touch_ends(result, stream_key, smallest, high):
    index_at = [jax.random.randint(jax.random.fold_in(stream_key, axis), (), 0, length) for axis, length in enumerate(result.shape)]
    longest = result.shape.index(max(result.shape))
    beside = index_at[:longest] + [(index_at[longest] + 1) % result.shape[longest]] + index_at[longest + 1:]
    return result.at[tuple(index_at)].set(smallest).at[tuple(beside)].set(high)


def level_of(key, dims, pieces, low, largest):
    def one(dim, shards_of):
        draws = jax.random.uniform(jax.random.fold_in(jax.random.fold_in(key, 6), dim), (shards_of,), jnp.float32, low / len(pieces), largest / len(pieces))
        return jnp.repeat(jnp.exp(draws), dims[dim] // shards_of).reshape((-1,) + (1,) * (len(dims) - dim - 1))

    gain = one(*pieces[0])
    for cut in pieces[1:]:
        gain = gain * one(*cut)
    return gain


def cumulative_ranks(number_of, lean):
    portions = [(1 << 20) // math.isqrt(grade ** lean) + 1 for grade in range(1, number_of + 1)]
    width = 1 + sum(portions) // (1 << 30)
    return np.cumsum(np.array([max(1, weight // width) for weight in portions]))


def ranked(rng, extent, amount, slope):
    table = cumulative_ranks(amount, slope)
    ticket = jax.random.randint(jax.random.fold_in(rng, 1), extent, 0, int(table[amount - 1]))
    grade = jnp.searchsorted(jnp.asarray(table, jnp.int32), ticket, side="right")
    return jax.random.permutation(jax.random.fold_in(rng, 2), amount)[grade].astype(jnp.int32)


def scatter_about(key, shape, width, reach, pieces=(), kind=jnp.bfloat16):
    array = jax.random.normal(key, shape, jnp.float32) * width
    if len(pieces) > 0:
        array = level_of(key, shape, pieces, -0.22, 0.18) * array
    return jnp.clip(array, min=-reach, max=reach).astype(kind)


def setup_inputs(seed: int = 0) -> dict:
    arg_keys = jax.random.split(jax.random.key(seed), 6)
    tokens = scatter_about(arg_keys[0], (TOKENS, D), 1.0, 6.0, ((0, 32),))
    token_ids = touch_ends(ranked(arg_keys[1], (TOKENS,), VOCAB, 2), jax.random.fold_in(arg_keys[1], 3), 0, VOCAB - 1).astype(jnp.int32)
    table = touch_ends(jax.random.randint(arg_keys[2], (VOCAB,), 0, EXPERTS), jax.random.fold_in(arg_keys[2], 1), 0, EXPERTS - 1).astype(jnp.int32)
    w_in = scatter_about(arg_keys[3], (EXPERTS, D, H), D ** -0.5, 0.125, ((0, 8), (2, 4)))
    w_out = scatter_about(arg_keys[4], (EXPERTS, H, D), H ** -0.5, 0.125, ((0, 8), (1, 4)))
    return {"tokens": tokens, "token_ids": token_ids, "table": table, "w_in": w_in, "w_out": w_out}


def reference(tokens, token_ids, table, w_in, w_out):
    blocks = N_EXPERT * N_PAIR
    quarter = H // N_PAIR
    chosen = jnp.take(table, token_ids, axis=0).astype(jnp.int32).reshape(blocks, TOK_DEV)
    hot = (chosen[:, :, None] == jnp.arange(EXPERTS, dtype=jnp.int32)[None, None, :]).astype(jnp.int32)
    earlier = jnp.cumsum(hot, axis=1) - hot
    rank = jnp.sum(earlier * hot, axis=2)
    kept = rank < CAP
    block_index = jnp.arange(blocks, dtype=jnp.int32)[:, None]
    total_slots = EXPERTS * blocks * CAP
    position = (chosen * blocks + block_index) * CAP + rank
    position = jnp.where(kept, position, total_slots).reshape(-1).astype(jnp.int32)
    buffer = jnp.zeros((total_slots, D), jnp.bfloat16).at[position].set(tokens, mode="drop")
    buffer = buffer.reshape(EXPERTS, blocks * CAP, D)

    def one_expert(items):
        rows, first, second = items
        hidden = jax.nn.relu(jnp.dot(rows, first, preferred_element_type=jnp.float32)).astype(jnp.bfloat16)
        total = jnp.zeros((rows.shape[0], D), jnp.float32)
        for index in range(N_PAIR):
            part = jnp.dot(hidden[:, index * quarter:(index + 1) * quarter],
                           second[index * quarter:(index + 1) * quarter],
                           preferred_element_type=jnp.float32).astype(jnp.bfloat16)
            total = total + lax.optimization_barrier(part).astype(jnp.float32)
        return total.astype(jnp.bfloat16)

    outputs = lax.map(one_expert, (buffer, w_in, w_out)).reshape(total_slots, D)
    safe = jnp.minimum(position, total_slots - 1).astype(jnp.int32)
    picked = jnp.take(outputs, safe, axis=0)
    mixed = jnp.where(kept.reshape(-1)[:, None], picked, jnp.zeros_like(picked))
    return mixed.astype(jnp.bfloat16)
```

```python
import functools

import jax
import jax.numpy as jnp
from jax import lax
from jax.experimental import pallas as pl
from jax.experimental.pallas import tpu as pltpu
from jax.sharding import PartitionSpec as P

ROWS = 16
TILE = 256
LANES = 128
MESH = pl.DeviceIdType.MESH


def exact_dot(a, b):
    return jnp.dot(a, b, preferred_element_type=jnp.float32)


def across(me, j):
    other = me
    bit = 1
    while bit <= j:
        if j & bit:
            other = other + bit * (1 - 2 * (me // bit % 2))
        bit *= 2
    return other


def places(shape, dim):
    return lax.broadcasted_iota(jnp.int32, shape, dim)


def one_hot(flags):
    return jnp.where(flags, 1.0, 0.0).astype(jnp.bfloat16)


def slot_of_token(ids, table, me, exp_local, n, slots, per_expert):
    tok = ids.shape[1]
    lines = table.astype(jnp.float32).astype(jnp.bfloat16)
    line = one_hot(places((lines.shape[0], tok), 0) == ids // LANES)
    found = lax.dot_general(
        lines, line, (((0,), (0,)), ((), ())), preferred_element_type=jnp.float32
    )
    lane = places((LANES, tok), 0) == ids % LANES
    chosen = jnp.sum(jnp.where(lane, found, 0.0), axis=0, keepdims=True).astype(jnp.int32)
    hot = places((exp_local * n, tok), 0) == chosen
    before = places((tok, tok), 0) < places((tok, tok), 1)
    earlier = exact_dot(one_hot(hot), one_hot(before))
    rank = jnp.sum(jnp.where(hot, earlier, 0.0), axis=0, keepdims=True).astype(jnp.int32)
    group = chosen // exp_local
    ahead = jnp.bitwise_xor(group, me)
    chunk = chosen % exp_local * per_expert + rank // ROWS
    return jnp.where(rank < slots, (chunk * n + ahead) * ROWS + rank % ROWS, -1)


def layer_kernel(
    n,
    slots,
    ids_in,
    table_in,
    tokens_in,
    w_in,
    w_out,
    result,
    ids,
    table,
    tokens,
    packed,
    back,
    column,
    mixed,
    first,
    second,
    rows,
    hidden,
    part,
    near,
    far,
    in_sem,
    out_sem,
    go_sem,
    come_sem,
    pair_go,
    pair_come,
    part_go,
    part_come,
    ret_go,
    ret_come,
):
    chunks, block, width = packed.shape
    exp_local = w_in.shape[0]
    per_expert = chunks // exp_local
    half = n // 2
    me = lax.axis_index("expert")
    at = lax.axis_index("pair")
    core = {"pair": at + 1 - 2 * (at % 2)}
    chip = {"pair": (at + 2) % 4}
    ahead = [{"expert": across(me, j)} for j in range(n)]

    loads = [
        pltpu.make_async_copy(src, dst, in_sem.at[k])
        for k, (src, dst) in enumerate(
            [(ids_in, ids), (table_in, table), (tokens_in, tokens), (w_in, first), (w_out, second)]
        )
    ]
    for copy in loads:
        copy.start()

    barrier = pltpu.get_barrier_semaphore()
    for peer in [core, chip] + ahead[1:]:
        pl.semaphore_signal(barrier, inc=1, device_id=peer, device_id_type=MESH)

    loads[0].wait()
    loads[1].wait()
    slot = slot_of_token(ids[...].reshape(1, ids.shape[0]), table[...], me, exp_local, n, slots, per_expert)
    tok = slot.shape[1]
    column[...] = jnp.transpose(jnp.broadcast_to(slot, (LANES, tok)))
    loads[2].wait()

    def copy_to(src, dst, send, recv, peer):
        return pltpu.make_async_remote_copy(
            src_ref=src,
            dst_ref=dst,
            send_sem=send,
            recv_sem=recv,
            device_id=peer,
            device_id_type=MESH,
        )

    def blocks(lo, hi):
        return pl.ds(lo * ROWS, (hi - lo) * ROWS)

    def span(c, lo, hi):
        return pl.ds(c * block + lo * ROWS, (hi - lo) * ROWS)

    own = blocks(0, 1)
    groups = [(1, 2), (2, half), (half, n)]
    group_of = [g for j in range(n) for g in range(3) if groups[g][0] <= max(j, 1) < groups[g][1]]
    bounds = [(0, half), (half, n)]

    def send_block(c, j):
        some = blocks(j, j + 1)
        recv = come_sem.at[c, group_of[j]]
        copy_to(packed.at[c, some], rows.at[c, 0, some], go_sem, recv, ahead[j]).start()

    def wait_blocks(c, g):
        some = blocks(*groups[g])
        copy_to(
            packed.at[c, some], rows.at[c, 0, some], go_sem, come_sem.at[c, g], ahead[1]
        ).wait_recv()

    def to_pair(kind, c, h, some, start):
        if kind == 0:
            src, dst, peer = rows.at[c, 0, some], rows.at[c, 2, some], chip
        elif kind == 1:
            src, dst, peer = rows.at[c, 0, some], rows.at[c, 1, some], core
        else:
            src, dst, peer = rows.at[c, 2, some], rows.at[c, 3, some], core
        copy = copy_to(src, dst, pair_go.at[kind], pair_come.at[kind, c, h], peer)
        if start:
            copy.start()
        else:
            copy.wait_recv()

    def spread(c, h, lo, hi):
        to_pair(0, c, h, blocks(lo, hi), True)
        to_pair(1, c, h, blocks(lo, hi), True)

    def pack(c):
        placer = one_hot(places((block, tok), 0) + c * block == slot)
        wide_tile = 4 * TILE

        def step(t, carry):
            cols = pl.ds(pl.multiple_of(t * wide_tile, wide_tile), wide_tile)
            x = exact_dot(placer, tokens[:, cols]).astype(jnp.bfloat16)
            packed[c, :, cols] = x
            rows[c, 0, own, cols] = x[:ROWS]
            return carry

        lax.fori_loop(0, width // wide_tile, step, 0)

    others = list(range(half, n)) + list(range(2, half))
    pack(0)
    pack(1)
    pl.semaphore_wait(barrier, n + 1)
    for c in range(chunks):
        if c > 1:
            pack(c)
        spread(c, 0, 0, 1)
        send_block(c, 1)
        if c == 0:
            for j in others:
                send_block(c, j)
    for c in range(1, chunks):
        for j in others:
            send_block(c, j)
    for c in range(chunks):
        wait_blocks(c, 0)
        spread(c, 0, 1, 2)

    def spread_rest(c, h):
        wait_blocks(c, 1 + h)
        spread(c, h, *groups[1 + h])

    def relay(c, h):
        to_pair(0, c, h, blocks(*bounds[h]), False)
        to_pair(2, c, h, blocks(*bounds[h]), True)

    def to_part(kind, c, p, some, start):
        if kind == 0:
            src, dst, peer = part.at[c, 3, some], near.at[c, 1, some], core
        elif kind == 1:
            src, dst, peer = part.at[c, 1, some], near.at[c, 0, some], core
        else:
            src, dst, peer = part.at[c, 2, some], far.at[c, some], chip
        copy = copy_to(src, dst, part_go.at[kind], part_come.at[kind, c, p], peer)
        if start:
            copy.start()
        else:
            copy.wait_recv()

    def compute(c, h):
        e = c // per_expert
        if (c, h) == units[0]:
            for copy in loads[3:]:
                copy.wait()
        some = blocks(*bounds[h])
        size = (bounds[h][1] - bounds[h][0]) * ROWS
        to_pair(1, c, h, some, False)
        to_pair(2, c, h, some, False)

        def project_in(t, carry):
            cols = pl.ds(pl.multiple_of(t * TILE, TILE), TILE)
            x = rows[c, :, some].reshape(4 * size, width)
            hid = exact_dot(x, first[e, :, cols])
            hidden[:, cols] = jnp.maximum(hid, 0.0).astype(jnp.bfloat16)
            return carry

        lax.fori_loop(0, first.shape[2] // TILE, project_in, 0)

        def project_out(t, carry):
            tile = 2 * TILE
            cols = pl.ds(pl.multiple_of(t * tile, tile), tile)
            y = exact_dot(hidden[...], second[e, :, cols]).astype(jnp.bfloat16)
            for k in range(4):
                part[c, k, some, cols] = y[k * size : (k + 1) * size]
            return carry

        lax.fori_loop(0, width // (2 * TILE), project_out, 0)
        to_part(0, c, h, some, True)
        to_part(1, c, h, some, True)

    def over_rows(lo, hi, body):
        def step(t, carry):
            body(pl.ds(pl.multiple_of(t * ROWS, ROWS), ROWS))
            return carry

        lax.fori_loop(lo, hi, step, 0)

    def wide(x):
        return x.astype(jnp.float32)

    def pieces(c, h):
        if (c, h) == units[-1]:
            return [(2, half, 0), (0, 2, 2)]
        return [bounds[h] + (h,)]

    def cross(c, h):
        to_part(0, c, h, blocks(*bounds[h]), False)
        for lo, hi, p in pieces(c, h):

            def add(r):
                both = wide(part[c, 2, r]) + wide(near[c, 1, r])
                part[c, 2, r] = both.astype(jnp.bfloat16)

            over_rows(lo, hi, add)
            to_part(2, c, p, blocks(lo, hi), True)

    def finish(c, h):
        to_part(1, c, h, blocks(*bounds[h]), False)
        for lo, hi, p in pieces(c, h):
            to_part(2, c, p, blocks(lo, hi), False)

            def add(r):
                both = wide(part[c, 0, r]) + wide(near[c, 0, r])
                both = both + wide(far[c, r])
                part[c, 0, r] = both.astype(jnp.bfloat16)

            over_rows(lo, hi, add)
            for j in range(max(lo, 1), hi):
                copy_to(
                    part.at[c, 0, blocks(j, j + 1)],
                    back.at[span(c, j, j + 1)],
                    ret_go,
                    ret_come.at[c, h],
                    ahead[j],
                ).start()
            if lo == 0:
                back[span(c, 0, 1)] = part[c, 0, own]

    def arrived(c, h):
        lo, hi = bounds[h]
        lo = max(lo, 1)
        copy_to(
            part.at[c, 0, blocks(lo, hi)],
            back.at[span(c, lo, hi)],
            ret_go,
            ret_come.at[c, h],
            ahead[1],
        ).wait_recv()

    def pick(ranges, more, store):
        picker = jnp.concatenate(
            [
                one_hot(column[:, : hi - lo] == places((tok, hi - lo), 1) + lo)
                for lo, hi in ranges
            ],
            axis=1,
        )

        tile = (2 if store else 4) * TILE

        def step(t, carry):
            some = pl.ds(pl.multiple_of(t * tile, tile), tile)
            x = jnp.concatenate([back[lo:hi, some] for lo, hi in ranges], axis=0)
            y = exact_dot(picker, x)
            if more:
                y = y + wide(mixed[:, some])
            mixed[:, some] = y.astype(jnp.bfloat16)
            return carry

        if store:
            for t in range(width // tile):
                step(t, 0)
                cols = pl.ds(t * tile, tile)
                copy = pltpu.make_async_copy(
                    mixed.at[:, cols], result.at[:, cols], out_sem.at[t]
                )
                copy.start()
                stores.append(copy)
        else:
            lax.fori_loop(0, width // tile, step, 0)

    units = unit_order(chunks)
    count = len(units)
    for i in range(count + 1):
        if i < count:
            spread_rest(*units[i])
        if i >= 1:
            relay(*units[i - 1])
            compute(*units[i - 1])
            cross(*units[i - 1])
        if i >= 2:
            finish(*units[i - 2])

    def slots_of(lo, hi):
        return [(c * block, (c + 1) * block) for c in range(lo, hi)]

    stores = []
    early = chunks // 2
    last = chunks - 1
    for c in range(early):
        arrived(c, 0)
        arrived(c, 1)
    pick(slots_of(0, early), False, False)
    arrived(early, 0)
    arrived(early, 1)
    finish(*units[-1])
    pick(slots_of(early, early + 1), True, False)
    for c in range(early + 1, last):
        arrived(c, 0)
        arrived(c, 1)
    arrived(last, 1)
    pick(slots_of(early + 1, last) + [(last * block + half * ROWS, chunks * block)], True, False)
    arrived(last, 0)
    pick([(last * block, last * block + half * ROWS)], True, True)

    every = rows.at[:, 0]
    but_own = pl.ds(ROWS, block - ROWS)
    copy_to(packed.at[:, but_own], rows.at[:, 0, but_own], go_sem, go_sem, core).wait_send()
    for kind in range(3):
        copy_to(every, every, pair_go.at[kind], go_sem, core).wait_send()
        copy_to(every, every, part_go.at[kind], go_sem, core).wait_send()
    copy_to(part.at[:, 0, but_own], rows.at[:, 0, but_own], ret_go, go_sem, core).wait_send()
    for copy in stores:
        copy.wait()


def unit_order(chunks):
    early = chunks // 2
    order = [(c, h) for c in range(early) for h in (1, 0)]
    order += [(c, 1) for c in range(early, chunks)]
    return order + [(c, 0) for c in range(early, chunks)]


def expert_layer(ids, table, tokens, w_in, w_out, n, slots):
    exp_local, width, quarter = w_in.shape
    tok = tokens.shape[0]
    chunks = exp_local * slots // ROWS
    block = n * ROWS
    bf16 = jnp.bfloat16
    dma = pltpu.SemaphoreType.DMA
    anywhere = pl.BlockSpec(memory_space=pl.ANY)
    return pl.pallas_call(
        functools.partial(layer_kernel, n, slots),
        out_shape=jax.ShapeDtypeStruct(tokens.shape, bf16),
        in_specs=[anywhere] * 5,
        out_specs=anywhere,
        scratch_shapes=[
            pltpu.VMEM(ids.shape, jnp.int32),
            pltpu.VMEM(table.shape, jnp.int32),
            pltpu.VMEM(tokens.shape, bf16),
            pltpu.VMEM((chunks, block, width), bf16),
            pltpu.VMEM((chunks * block, width), bf16),
            pltpu.VMEM((tok, LANES), jnp.int32),
            pltpu.VMEM(tokens.shape, bf16),
            pltpu.VMEM(w_in.shape, bf16),
            pltpu.VMEM(w_out.shape, bf16),
            pltpu.VMEM((chunks, 4, block, width), bf16),
            pltpu.VMEM((2 * block, quarter), bf16),
            pltpu.VMEM((chunks, 4, block, width), bf16),
            pltpu.VMEM((chunks, 2, block, width), bf16),
            pltpu.VMEM((chunks, block, width), bf16),
            dma((5,)),
            dma((width // TILE,)),
            dma,
            dma((chunks, 3)),
            dma((3,)),
            dma((3, chunks, 2)),
            dma((3,)),
            dma((3, chunks, 3)),
            dma,
            dma((chunks, 2)),
        ],
        compiler_params=pltpu.CompilerParams(
            collective_id=0, has_side_effects=True, vmem_limit_bytes=62 * 1024 * 1024
        ),
    )(ids, table, tokens, w_in, w_out)


def plain(tokens, token_ids, table, w_in, w_out):
    groups = lax.axis_size("expert")
    exp_local = w_in.shape[0]
    experts = groups * exp_local
    tok_rows, width = tokens.shape
    slots = max(2, 2 * tok_rows // experts)
    quarter = w_out.shape[1]
    chosen = jnp.take(table, token_ids, axis=0)
    expert_hot = (chosen[:, None] == jnp.arange(experts, dtype=jnp.int32)[None, :]).astype(
        jnp.int32
    )
    earlier = jnp.cumsum(expert_hot, axis=0) - expert_hot
    rank_tok = jnp.sum(earlier * expert_hot, axis=1)
    kept = rank_tok < slots
    column = (chosen // exp_local * slots + rank_tok) * exp_local + chosen % exp_local
    placer = (
        (column[:, None] == jnp.arange(experts * slots, dtype=jnp.int32)[None, :]) & kept[:, None]
    ).astype(jnp.bfloat16)
    packed = jnp.einsum("ts,td->sd", placer, tokens, preferred_element_type=jnp.float32).astype(
        jnp.bfloat16
    )
    packed = packed.reshape(groups * slots, exp_local, width)
    arrived = lax.all_to_all(packed, "expert", split_axis=0, concat_axis=0, tiled=True)
    rows = arrived.shape[0]
    hidden = jax.nn.relu(
        jnp.einsum(
            "red,edh->reh",
            arrived,
            lax.all_gather(w_in, "pair", axis=2, tiled=True),
            preferred_element_type=jnp.float32,
        )
    ).astype(jnp.bfloat16)
    total = jnp.zeros((rows, exp_local, width), jnp.float32)
    piece = lax.all_gather(w_out, "pair", axis=1, tiled=True)
    for index in range(piece.shape[1] // quarter):
        cols = lax.dynamic_slice_in_dim(hidden, index * quarter, quarter, 2)
        part = jnp.einsum(
            "reh,ehd->red",
            cols,
            piece[:, index * quarter : (index + 1) * quarter],
            preferred_element_type=jnp.float32,
        ).astype(jnp.bfloat16)
        total = total + lax.optimization_barrier(part).astype(jnp.float32)
    result = total.astype(jnp.bfloat16)
    returned = lax.all_to_all(result, "expert", split_axis=0, concat_axis=0, tiled=True)
    flat = returned.reshape(experts * slots, width)
    return jnp.dot(placer, flat, preferred_element_type=jnp.float32).astype(jnp.bfloat16)


def on_device(tokens, token_ids, table, w_in, w_out):
    n = lax.axis_size("expert")
    exp_local = w_in.shape[0]
    experts = n * exp_local
    tok_rows, width = tokens.shape
    slots = max(2, 2 * tok_rows // experts)
    fits = slots % ROWS == 0 and tok_rows % LANES == 0 and table.shape[0] % LANES == 0
    fits = fits and lax.axis_size("pair") == 4 and experts <= 256 and n == LANES // ROWS
    fits = fits and width % (4 * TILE) == 0 and w_in.shape[2] % TILE == 0
    if not fits or exp_local * slots // ROWS < 3:
        return plain(tokens, token_ids, table, w_in, w_out)
    return expert_layer(
        token_ids, table.reshape(-1, LANES), tokens, w_in, w_out, n, slots
    )


def solution(mesh):
    in_specs = (
        P(("expert", "pair"), None),
        P(("expert", "pair")),
        P(),
        P("expert", None, "pair"),
        P("expert", "pair", None),
    )
    out_specs = P(("expert", "pair"), None)
    return jax.shard_map(
        on_device, mesh=mesh, in_specs=in_specs, out_specs=out_specs, check_vma=False
    )
```

```python
import functools

import jax
import jax.numpy as jnp
from jax import lax
from jax.experimental import pallas as pl
from jax.experimental.pallas import tpu as pltpu
from jax.sharding import PartitionSpec as P

ROWS = 16
TILE = 256
LANES = 128
MESH = pl.DeviceIdType.MESH


def exact_dot(a, b):
    return jnp.dot(a, b, preferred_element_type=jnp.float32)


def across(me, j):
    other = me
    bit = 1
    while bit <= j:
        if j & bit:
            other = other + bit * (1 - 2 * (me // bit % 2))
        bit *= 2
    return other


def places(shape, dim):
    return lax.broadcasted_iota(jnp.int32, shape, dim)


def one_hot(flags):
    return jnp.where(flags, 1.0, 0.0).astype(jnp.bfloat16)


def slot_of_token(ids, table, me, exp_local, n, slots, per_expert):
    tok = ids.shape[1]
    lines = table.astype(jnp.float32).astype(jnp.bfloat16)
    line = one_hot(places((lines.shape[0], tok), 0) == ids // LANES)
    found = lax.dot_general(
        lines, line, (((0,), (0,)), ((), ())), preferred_element_type=jnp.float32
    )
    lane = places((LANES, tok), 0) == ids % LANES
    chosen = jnp.sum(jnp.where(lane, found, 0.0), axis=0, keepdims=True).astype(jnp.int32)
    hot = places((exp_local * n, tok), 0) == chosen
    before = places((tok, tok), 0) < places((tok, tok), 1)
    earlier = exact_dot(one_hot(hot), one_hot(before))
    rank = jnp.sum(jnp.where(hot, earlier, 0.0), axis=0, keepdims=True).astype(jnp.int32)
    group = chosen // exp_local
    ahead = jnp.bitwise_xor(group, me)
    chunk = chosen % exp_local * per_expert + rank // ROWS
    return jnp.where(rank < slots, (chunk * n + ahead) * ROWS + rank % ROWS, -1)


def layer_kernel(
    n,
    slots,
    ids_in,
    table_in,
    tokens_in,
    w_in,
    w_out,
    result,
    ids,
    table,
    tokens,
    packed,
    back,
    column,
    mixed,
    first,
    second,
    rows,
    hidden,
    part,
    near,
    far,
    in_sem,
    out_sem,
    go_sem,
    come_sem,
    pair_go,
    pair_come,
    part_go,
    part_come,
    ret_go,
    ret_come,
):
    chunks, block, width = packed.shape
    exp_local = w_in.shape[0]
    per_expert = chunks // exp_local
    half = n // 2
    me = lax.axis_index("expert")
    at = lax.axis_index("pair")
    core = {"pair": at + 1 - 2 * (at % 2)}
    chip = {"pair": (at + 2) % 4}
    ahead = [{"expert": across(me, j)} for j in range(n)]

    loads = [
        pltpu.make_async_copy(src, dst, in_sem.at[k])
        for k, (src, dst) in enumerate(
            [(ids_in, ids), (table_in, table), (tokens_in, tokens), (w_in, first), (w_out, second)]
        )
    ]
    for copy in loads:
        copy.start()

    barrier = pltpu.get_barrier_semaphore()
    for peer in [core, chip] + ahead[1:]:
        pl.semaphore_signal(barrier, inc=1, device_id=peer, device_id_type=MESH)

    loads[0].wait()
    loads[1].wait()
    slot = slot_of_token(ids[...].reshape(1, ids.shape[0]), table[...], me, exp_local, n, slots, per_expert)
    tok = slot.shape[1]
    column[...] = jnp.transpose(jnp.broadcast_to(slot, (LANES, tok)))
    loads[2].wait()

    def copy_to(src, dst, send, recv, peer):
        return pltpu.make_async_remote_copy(
            src_ref=src,
            dst_ref=dst,
            send_sem=send,
            recv_sem=recv,
            device_id=peer,
            device_id_type=MESH,
        )

    def blocks(lo, hi):
        return pl.ds(lo * ROWS, (hi - lo) * ROWS)

    def span(c, lo, hi):
        return pl.ds(c * block + lo * ROWS, (hi - lo) * ROWS)

    own = blocks(0, 1)
    groups = [(1, 2), (2, half), (half, n)]
    group_of = [g for j in range(n) for g in range(3) if groups[g][0] <= max(j, 1) < groups[g][1]]
    bounds = [(0, half), (half, n)]

    def send_block(c, j):
        some = blocks(j, j + 1)
        recv = come_sem.at[c, group_of[j]]
        copy_to(packed.at[c, some], rows.at[c, 0, some], go_sem, recv, ahead[j]).start()

    def wait_blocks(c, g):
        some = blocks(*groups[g])
        copy_to(
            packed.at[c, some], rows.at[c, 0, some], go_sem, come_sem.at[c, g], ahead[1]
        ).wait_recv()

    def to_pair(kind, c, h, some, start):
        if kind == 0:
            src, dst, peer = rows.at[c, 0, some], rows.at[c, 2, some], chip
        elif kind == 1:
            src, dst, peer = rows.at[c, 0, some], rows.at[c, 1, some], core
        else:
            src, dst, peer = rows.at[c, 2, some], rows.at[c, 3, some], core
        copy = copy_to(src, dst, pair_go.at[kind], pair_come.at[kind, c, h], peer)
        if start:
            copy.start()
        else:
            copy.wait_recv()

    def spread(c, h, lo, hi):
        to_pair(0, c, h, blocks(lo, hi), True)
        to_pair(1, c, h, blocks(lo, hi), True)

    def pack(c):
        placer = one_hot(places((block, tok), 0) + c * block == slot)
        wide_tile = 4 * TILE

        def step(t, carry):
            cols = pl.ds(pl.multiple_of(t * wide_tile, wide_tile), wide_tile)
            x = exact_dot(placer, tokens[:, cols]).astype(jnp.bfloat16)
            packed[c, :, cols] = x
            rows[c, 0, own, cols] = x[:ROWS]
            return carry

        lax.fori_loop(0, width // wide_tile, step, 0)

    early, steps, spreads = plan(chunks)

    def dispatch(c, h):
        for j in range(*groups[1 + h]):
            send_block(c, j)

    pack(0)
    pack(1)
    pl.semaphore_wait(barrier, n + 1)
    for c in range(chunks):
        if c > 1:
            pack(c)
        spread(c, 0, 0, 1)
        send_block(c, 1)
        dispatch(c, 0)
        if c == 0:
            dispatch(0, 1)
    for c in range(1, chunks):
        dispatch(c, 1)
    def spread_rest(c, h):
        wait_blocks(c, 1 + h)
        spread(c, h, *groups[1 + h])

    def spread_beside(c):
        wait_blocks(c, 0)
        spread(c, 0, 1, 2)

    def relay(c, h):
        to_pair(0, c, h, blocks(*bounds[h]), False)
        to_pair(2, c, h, blocks(*bounds[h]), True)

    def to_part(kind, c, p, some, start):
        if kind == 0:
            src, dst, peer = part.at[c, 3, some], near.at[c, 1, some], core
        elif kind == 1:
            src, dst, peer = part.at[c, 1, some], near.at[c, 0, some], core
        else:
            src, dst, peer = part.at[c, 2, some], far.at[c, some], chip
        copy = copy_to(src, dst, part_go.at[kind], part_come.at[kind, c, p], peer)
        if start:
            copy.start()
        else:
            copy.wait_recv()

    def compute(c, h):
        e = c // per_expert
        if (c, h) == steps[0]:
            for copy in loads[3:]:
                copy.wait()
        some = blocks(*bounds[h])
        size = (bounds[h][1] - bounds[h][0]) * ROWS
        to_pair(1, c, h, some, False)
        to_pair(2, c, h, some, False)

        def project_in(t, carry):
            cols = pl.ds(pl.multiple_of(t * TILE, TILE), TILE)
            x = rows[c, :, some].reshape(4 * size, width)
            hid = exact_dot(x, first[e, :, cols])
            hidden[:, cols] = jnp.maximum(hid, 0.0).astype(jnp.bfloat16)
            return carry

        lax.fori_loop(0, first.shape[2] // TILE, project_in, 0)

        def project_out(t, carry):
            tile = 2 * TILE
            cols = pl.ds(pl.multiple_of(t * tile, tile), tile)
            y = exact_dot(hidden[...], second[e, :, cols]).astype(jnp.bfloat16)
            for k in range(4):
                part[c, k, some, cols] = y[k * size : (k + 1) * size]
            return carry

        lax.fori_loop(0, width // (2 * TILE), project_out, 0)
        to_part(0, c, h, some, True)
        to_part(1, c, h, some, True)

    def over_rows(lo, hi, body):
        def step(t, carry):
            body(pl.ds(pl.multiple_of(t * ROWS, ROWS), ROWS))
            return carry

        lax.fori_loop(lo, hi, step, 0)

    def wide(x):
        return x.astype(jnp.float32)

    def pieces(c, h):
        if (c, h) == steps[-1]:
            return [(2, half, 0), (1, 2, 2), (0, 1, 3)]
        return [bounds[h] + (h,)]

    def cross(c, h):
        to_part(0, c, h, blocks(*bounds[h]), False)
        for lo, hi, p in pieces(c, h):

            def add(r):
                both = wide(part[c, 2, r]) + wide(near[c, 1, r])
                part[c, 2, r] = both.astype(jnp.bfloat16)

            over_rows(lo, hi, add)
            to_part(2, c, p, blocks(lo, hi), True)

    def finish(c, h):
        to_part(1, c, h, blocks(*bounds[h]), False)
        for lo, hi, p in pieces(c, h):
            to_part(2, c, p, blocks(lo, hi), False)

            def add(r):
                both = wide(part[c, 0, r]) + wide(near[c, 0, r])
                both = both + wide(far[c, r])
                part[c, 0, r] = both.astype(jnp.bfloat16)

            over_rows(lo, hi, add)
            for j in range(max(lo, 1), hi):
                copy_to(
                    part.at[c, 0, blocks(j, j + 1)],
                    back.at[span(c, j, j + 1)],
                    ret_go,
                    ret_come.at[c, h],
                    ahead[j],
                ).start()
            if lo == 0:
                back[span(c, 0, 1)] = part[c, 0, own]

    def arrived(c, h):
        lo, hi = bounds[h]
        lo = max(lo, 1)
        copy_to(
            part.at[c, 0, blocks(lo, hi)],
            back.at[span(c, lo, hi)],
            ret_go,
            ret_come.at[c, h],
            ahead[1],
        ).wait_recv()

    def pick(ranges, more, store):
        picker = jnp.concatenate(
            [
                one_hot(column[:, : hi - lo] == places((tok, hi - lo), 1) + lo)
                for lo, hi in ranges
            ],
            axis=1,
        )

        tile = (2 if store else 4) * TILE

        def step(t, carry):
            some = pl.ds(pl.multiple_of(t * tile, tile), tile)
            x = jnp.concatenate([back[lo:hi, some] for lo, hi in ranges], axis=0)
            y = exact_dot(picker, x)
            if more:
                y = y + wide(mixed[:, some])
            (result if store else mixed)[:, some] = y.astype(jnp.bfloat16)
            return carry

        if store:
            for t in range(width // tile):
                step(t, 0)
        else:
            lax.fori_loop(0, width // tile, step, 0)

    for c in range(early):
        spread_beside(c)
        spread_rest(c, 0)
    for i, (c, h) in enumerate(steps):
        relay(c, h)
        compute(c, h)
        cross(c, h)
        if i == 0:
            for late in range(early, chunks):
                spread_beside(late)
        else:
            finish(*steps[i - 1])
        if spreads[i]:
            spread_rest(*spreads[i])

    def slots_of(lo, hi):
        return [(c * block, (c + 1) * block) for c in range(lo, hi)]

    stores = []
    last = chunks - 1
    for c in range(early):
        arrived(c, 0)
        arrived(c, 1)
    pick(slots_of(0, early), False, False)
    arrived(early, 0)
    arrived(early, 1)
    finish(*steps[-1])
    pick(slots_of(early, early + 1), True, False)
    for c in range(early + 1, last):
        arrived(c, 0)
        arrived(c, 1)
    arrived(last, 1)
    pick(slots_of(early + 1, last) + [(last * block + half * ROWS, chunks * block)], True, False)
    every = rows.at[:, 0]
    but_own = pl.ds(ROWS, block - ROWS)
    copy_to(packed.at[:, but_own], rows.at[:, 0, but_own], go_sem, go_sem, core).wait_send()
    for kind in range(3):
        copy_to(every, every, pair_go.at[kind], go_sem, core).wait_send()
        copy_to(every, every, part_go.at[kind], go_sem, core).wait_send()
    copy_to(part.at[:, 0, but_own], rows.at[:, 0, but_own], ret_go, go_sem, core).wait_send()
    arrived(last, 0)
    pick([(last * block, last * block + half * ROWS)], True, True)


def plan(chunks):
    early = chunks // 2
    steps = [(0, 0)]
    for c in range(1, early):
        steps += [(c, 0), (c - 1, 1)]
    steps += [(c, 1) for c in range(early - 1, chunks)]
    steps += [(c, 0) for c in range(early, chunks)]
    spreads = [(c, 1) for c in range(chunks)] + [(c, 0) for c in range(early, chunks)]
    ahead = []
    for c, h in steps:
        wanted = h == 1 or not 2 <= c < early
        ahead.append(spreads.pop(0) if spreads and wanted else None)
    return early, steps, ahead


def expert_layer(ids, table, tokens, w_in, w_out, n, slots):
    exp_local, width, quarter = w_in.shape
    tok = tokens.shape[0]
    chunks = exp_local * slots // ROWS
    block = n * ROWS
    bf16 = jnp.bfloat16
    dma = pltpu.SemaphoreType.DMA
    anywhere = pl.BlockSpec(memory_space=pl.ANY)
    return pl.pallas_call(
        functools.partial(layer_kernel, n, slots),
        out_shape=pltpu.VMEM(tokens.shape, bf16),
        in_specs=[anywhere] * 5,
        out_specs=pl.BlockSpec(memory_space=pltpu.VMEM),
        scratch_shapes=[
            pltpu.VMEM(ids.shape, jnp.int32),
            pltpu.VMEM(table.shape, jnp.int32),
            pltpu.VMEM(tokens.shape, bf16),
            pltpu.VMEM((chunks, block, width), bf16),
            pltpu.VMEM((chunks * block, width), bf16),
            pltpu.VMEM((tok, LANES), jnp.int32),
            pltpu.VMEM(tokens.shape, bf16),
            pltpu.VMEM(w_in.shape, bf16),
            pltpu.VMEM(w_out.shape, bf16),
            pltpu.VMEM((chunks, 4, block, width), bf16),
            pltpu.VMEM((2 * block, quarter), bf16),
            pltpu.VMEM((chunks, 4, block, width), bf16),
            pltpu.VMEM((chunks, 2, block, width), bf16),
            pltpu.VMEM((chunks, block, width), bf16),
            dma((5,)),
            dma((width // TILE,)),
            dma,
            dma((chunks, 3)),
            dma((3,)),
            dma((3, chunks, 2)),
            dma((3,)),
            dma((3, chunks, 4)),
            dma,
            dma((chunks, 2)),
        ],
        compiler_params=pltpu.CompilerParams(
            collective_id=0, has_side_effects=True, vmem_limit_bytes=60 * 1024 * 1024
        ),
    )(ids, table, tokens, w_in, w_out)


def plain(tokens, token_ids, table, w_in, w_out):
    groups = lax.axis_size("expert")
    exp_local = w_in.shape[0]
    experts = groups * exp_local
    tok_rows, width = tokens.shape
    slots = max(2, 2 * tok_rows // experts)
    quarter = w_out.shape[1]
    chosen = jnp.take(table, token_ids, axis=0)
    expert_hot = (chosen[:, None] == jnp.arange(experts, dtype=jnp.int32)[None, :]).astype(
        jnp.int32
    )
    earlier = jnp.cumsum(expert_hot, axis=0) - expert_hot
    rank_tok = jnp.sum(earlier * expert_hot, axis=1)
    kept = rank_tok < slots
    column = (chosen // exp_local * slots + rank_tok) * exp_local + chosen % exp_local
    placer = (
        (column[:, None] == jnp.arange(experts * slots, dtype=jnp.int32)[None, :]) & kept[:, None]
    ).astype(jnp.bfloat16)
    packed = jnp.einsum("ts,td->sd", placer, tokens, preferred_element_type=jnp.float32).astype(
        jnp.bfloat16
    )
    packed = packed.reshape(groups * slots, exp_local, width)
    arrived = lax.all_to_all(packed, "expert", split_axis=0, concat_axis=0, tiled=True)
    rows = arrived.shape[0]
    hidden = jax.nn.relu(
        jnp.einsum(
            "red,edh->reh",
            arrived,
            lax.all_gather(w_in, "pair", axis=2, tiled=True),
            preferred_element_type=jnp.float32,
        )
    ).astype(jnp.bfloat16)
    total = jnp.zeros((rows, exp_local, width), jnp.float32)
    piece = lax.all_gather(w_out, "pair", axis=1, tiled=True)
    for index in range(piece.shape[1] // quarter):
        cols = lax.dynamic_slice_in_dim(hidden, index * quarter, quarter, 2)
        part = jnp.einsum(
            "reh,ehd->red",
            cols,
            piece[:, index * quarter : (index + 1) * quarter],
            preferred_element_type=jnp.float32,
        ).astype(jnp.bfloat16)
        total = total + lax.optimization_barrier(part).astype(jnp.float32)
    result = total.astype(jnp.bfloat16)
    returned = lax.all_to_all(result, "expert", split_axis=0, concat_axis=0, tiled=True)
    flat = returned.reshape(experts * slots, width)
    return jnp.dot(placer, flat, preferred_element_type=jnp.float32).astype(jnp.bfloat16)


def on_device(tokens, token_ids, table, w_in, w_out):
    n = lax.axis_size("expert")
    exp_local = w_in.shape[0]
    experts = n * exp_local
    tok_rows, width = tokens.shape
    slots = max(2, 2 * tok_rows // experts)
    fits = slots % ROWS == 0 and tok_rows % LANES == 0 and table.shape[0] % LANES == 0
    fits = fits and lax.axis_size("pair") == 4 and experts <= 256 and n == LANES // ROWS
    fits = fits and width % (4 * TILE) == 0 and w_in.shape[2] % TILE == 0
    if not fits or exp_local * slots // ROWS < 3:
        return plain(tokens, token_ids, table, w_in, w_out)
    return expert_layer(
        token_ids, table.reshape(-1, LANES), tokens, w_in, w_out, n, slots
    )


def solution(mesh):
    in_specs = (
        P(("expert", "pair"), None),
        P(("expert", "pair")),
        P(),
        P("expert", None, "pair"),
        P("expert", "pair", None),
    )
    out_specs = P(("expert", "pair"), None)
    return jax.shard_map(
        on_device, mesh=mesh, in_specs=in_specs, out_specs=out_specs, check_vma=False
    )
```

```python
import functools

import jax
import jax.numpy as jnp
from jax import lax
from jax.experimental import pallas as pl
from jax.experimental.pallas import tpu as pltpu
from jax.sharding import PartitionSpec as P

ROWS = 16
TILE = 256
LANES = 128
MESH = pl.DeviceIdType.MESH


def exact_dot(a, b):
    return jnp.dot(a, b, preferred_element_type=jnp.float32)


def across(me, j):
    other = me
    bit = 1
    while bit <= j:
        if j & bit:
            other = other + bit * (1 - 2 * (me // bit % 2))
        bit *= 2
    return other


def places(shape, dim):
    return lax.broadcasted_iota(jnp.int32, shape, dim)


def one_hot(flags):
    return jnp.where(flags, 1.0, 0.0).astype(jnp.bfloat16)


def slot_of_token(ids, table, me, exp_local, n, slots, per_expert):
    tok = ids.shape[1]
    lines = table.astype(jnp.float32).astype(jnp.bfloat16)
    line = one_hot(places((lines.shape[0], tok), 0) == ids // LANES)
    found = lax.dot_general(
        lines, line, (((0,), (0,)), ((), ())), preferred_element_type=jnp.float32
    )
    lane = places((LANES, tok), 0) == ids % LANES
    chosen = jnp.sum(jnp.where(lane, found, 0.0), axis=0, keepdims=True).astype(jnp.int32)
    hot = places((exp_local * n, tok), 0) == chosen
    before = places((tok, tok), 0) < places((tok, tok), 1)
    earlier = exact_dot(one_hot(hot), one_hot(before))
    rank = jnp.sum(jnp.where(hot, earlier, 0.0), axis=0, keepdims=True).astype(jnp.int32)
    group = chosen // exp_local
    ahead = jnp.bitwise_xor(group, me)
    chunk = chosen % exp_local * per_expert + rank // ROWS
    return jnp.where(rank < slots, (chunk * n + ahead) * ROWS + rank % ROWS, -1)


def layer_kernel(
    n,
    slots,
    ids_in,
    table_in,
    tokens_in,
    w_in,
    w_out,
    result,
    ids,
    table,
    tokens,
    packed,
    back,
    column,
    mixed,
    first,
    second,
    rows,
    hidden,
    part,
    near,
    far,
    in_sem,
    go_sem,
    come_sem,
    pair_go,
    pair_come,
    part_go,
    part_come,
    far_come,
    ret_go,
    ret_come,
):
    chunks, block, width = packed.shape
    exp_local = w_in.shape[0]
    per_expert = chunks // exp_local
    half = n // 2
    me = lax.axis_index("expert")
    at = lax.axis_index("pair")
    core = {"pair": at + 1 - 2 * (at % 2)}
    chip = {"pair": (at + 2) % 4}
    ahead = [{"expert": across(me, j)} for j in range(n)]

    loads = [
        pltpu.make_async_copy(src, dst, in_sem.at[k])
        for k, (src, dst) in enumerate(
            [(ids_in, ids), (table_in, table), (tokens_in, tokens), (w_in, first), (w_out, second)]
        )
    ]
    for copy in loads:
        copy.start()

    barrier = pltpu.get_barrier_semaphore()
    for peer in [core, chip] + ahead[1:]:
        pl.semaphore_signal(barrier, inc=1, device_id=peer, device_id_type=MESH)

    loads[0].wait()
    loads[1].wait()
    slot = slot_of_token(ids[...].reshape(1, ids.shape[0]), table[...], me, exp_local, n, slots, per_expert)
    tok = slot.shape[1]
    column[...] = jnp.transpose(jnp.broadcast_to(slot, (LANES, tok)))
    loads[2].wait()

    def copy_to(src, dst, send, recv, peer):
        return pltpu.make_async_remote_copy(
            src_ref=src,
            dst_ref=dst,
            send_sem=send,
            recv_sem=recv,
            device_id=peer,
            device_id_type=MESH,
        )

    def blocks(lo, hi):
        return pl.ds(lo * ROWS, (hi - lo) * ROWS)

    def span(c, lo, hi):
        return pl.ds(c * block + lo * ROWS, (hi - lo) * ROWS)

    own = blocks(0, 1)
    groups = [(1, 2), (2, half), (half, n)]
    group_of = [g for j in range(n) for g in range(3) if groups[g][0] <= max(j, 1) < groups[g][1]]
    bounds = [(0, half), (half, n)]

    def send_block(c, j):
        some = blocks(j, j + 1)
        recv = come_sem.at[c, group_of[j]]
        copy_to(packed.at[c, some], rows.at[c, 0, some], go_sem, recv, ahead[j]).start()

    def wait_blocks(c, g):
        some = blocks(*groups[g])
        copy_to(
            packed.at[c, some], rows.at[c, 0, some], go_sem, come_sem.at[c, g], ahead[1]
        ).wait_recv()

    def to_pair(kind, c, h, some, start):
        if kind == 0:
            src, dst, peer = rows.at[c, 0, some], rows.at[c, 2, some], chip
        elif kind == 1:
            src, dst, peer = rows.at[c, 0, some], rows.at[c, 1, some], core
        else:
            src, dst, peer = rows.at[c, 2, some], rows.at[c, 3, some], core
        copy = copy_to(src, dst, pair_go.at[kind], pair_come.at[kind, c, h], peer)
        if start:
            copy.start()
        else:
            copy.wait_recv()

    def spread(c, h, lo, hi):
        to_pair(0, c, h, blocks(lo, hi), True)
        to_pair(1, c, h, blocks(lo, hi), True)

    def pack(c):
        placer = one_hot(places((block, tok), 0) + c * block == slot)
        wide_tile = 4 * TILE

        def step(t, carry):
            cols = pl.ds(pl.multiple_of(t * wide_tile, wide_tile), wide_tile)
            x = exact_dot(placer, tokens[:, cols]).astype(jnp.bfloat16)
            packed[c, :, cols] = x
            rows[c, 0, own, cols] = x[:ROWS]
            return carry

        lax.fori_loop(0, width // wide_tile, step, 0)

    early, steps, spreads = plan(chunks)

    def dispatch(c, h):
        for j in range(*groups[1 + h]):
            send_block(c, j)

    pack(0)
    pack(1)
    pl.semaphore_wait(barrier, n + 1)
    for c in range(chunks):
        if c > 1:
            pack(c)
        spread(c, 0, 0, 1)
        send_block(c, 1)
        dispatch(c, 0)
        if c == 0:
            dispatch(0, 1)
    for c in range(1, chunks):
        dispatch(c, 1)
    def spread_rest(c, h):
        wait_blocks(c, 1 + h)
        spread(c, h, *groups[1 + h])

    def spread_beside(c):
        wait_blocks(c, 0)
        spread(c, 0, 1, 2)

    def relay(c, h):
        to_pair(0, c, h, blocks(*bounds[h]), False)
        to_pair(2, c, h, blocks(*bounds[h]), True)

    def to_part(kind, c, p, some, start):
        if kind == 0:
            src, dst, peer = part.at[c, 3, some], near.at[c, 1, some], core
        elif kind == 1:
            src, dst, peer = part.at[c, 1, some], near.at[c, 0, some], core
        else:
            src, dst, peer = part.at[c, 2, some], far.at[c, some], chip
        recv = far_come.at[c, p] if kind == 2 else part_come.at[kind, c, p]
        copy = copy_to(src, dst, part_go.at[kind], recv, peer)
        if start:
            copy.start()
        else:
            copy.wait_recv()

    def compute(c, h):
        e = c // per_expert
        if (c, h) == steps[0]:
            for copy in loads[3:]:
                copy.wait()
        some = blocks(*bounds[h])
        size = (bounds[h][1] - bounds[h][0]) * ROWS
        to_pair(1, c, h, some, False)
        to_pair(2, c, h, some, False)

        def project_in(t, carry):
            cols = pl.ds(pl.multiple_of(t * TILE, TILE), TILE)
            x = rows[c, :, some].reshape(4 * size, width)
            hid = exact_dot(x, first[e, :, cols])
            hidden[:, cols] = jnp.maximum(hid, 0.0).astype(jnp.bfloat16)
            return carry

        lax.fori_loop(0, first.shape[2] // TILE, project_in, 0)

        def project_out(t, carry):
            tile = 2 * TILE
            cols = pl.ds(pl.multiple_of(t * tile, tile), tile)
            y = exact_dot(hidden[...], second[e, :, cols]).astype(jnp.bfloat16)
            for k in range(4):
                part[c, k, some, cols] = y[k * size : (k + 1) * size]
            return carry

        lax.fori_loop(0, width // (2 * TILE), project_out, 0)
        to_part(0, c, h, some, True)
        to_part(1, c, h, some, True)

    def over_rows(lo, hi, body):
        def step(t, carry):
            body(pl.ds(pl.multiple_of(t * ROWS, ROWS), ROWS))
            return carry

        lax.fori_loop(lo, hi, step, 0)

    def wide(x):
        return x.astype(jnp.float32)

    def pieces(c, h):
        if h == 0 and c >= early:
            return [(2, half, 0), (1, 2, 2)]
        return [bounds[h] + (h,)]

    def cross(c, h):
        to_part(0, c, h, blocks(*bounds[h]), False)

        def add(r):
            both = wide(part[c, 2, r]) + wide(near[c, 1, r])
            part[c, 2, r] = both.astype(jnp.bfloat16)

        for lo, hi, p in pieces(c, h):
            over_rows(lo, hi, add)
            to_part(2, c, p, blocks(lo, hi), True)

    def cross_own(c):
        both = wide(part[c, 2, own]) + wide(near[c, 1, own])
        part[c, 2, own] = both.astype(jnp.bfloat16)
        to_part(2, c, 3, own, True)

    def sum_up(c, r):
        both = wide(part[c, 0, r]) + wide(near[c, 0, r])
        return (both + wide(far[c, r])).astype(jnp.bfloat16)

    def finish_own(c):
        to_part(2, c, 3, own, False)
        back[span(c, 0, 1)] = sum_up(c, own)

    def finish(c, h):
        to_part(1, c, h, blocks(*bounds[h]), False)
        for lo, hi, p in pieces(c, h):
            to_part(2, c, p, blocks(lo, hi), False)

            def add(r):
                part[c, 0, r] = sum_up(c, r)

            over_rows(lo, hi, add)
            for j in range(max(lo, 1), hi):
                copy_to(
                    part.at[c, 0, blocks(j, j + 1)],
                    back.at[span(c, j, j + 1)],
                    ret_go,
                    ret_come.at[c, h],
                    ahead[j],
                ).start()
            if lo == 0:
                back[span(c, 0, 1)] = part[c, 0, own]

    def arrived(c, h):
        lo, hi = bounds[h]
        lo = max(lo, 1)
        copy_to(
            part.at[c, 0, blocks(lo, hi)],
            back.at[span(c, lo, hi)],
            ret_go,
            ret_come.at[c, h],
            ahead[1],
        ).wait_recv()

    def pick(ranges, more, store):
        picker = jnp.concatenate(
            [
                one_hot(column[:, : hi - lo] == places((tok, hi - lo), 1) + lo)
                for lo, hi in ranges
            ],
            axis=1,
        )

        tile = (2 if store else 4) * TILE

        def step(t, carry):
            some = pl.ds(pl.multiple_of(t * tile, tile), tile)
            x = jnp.concatenate([back[lo:hi, some] for lo, hi in ranges], axis=0)
            y = exact_dot(picker, x)
            if more:
                y = y + wide(mixed[:, some])
            (result if store else mixed)[:, some] = y.astype(jnp.bfloat16)
            return carry

        if store:
            for t in range(width // tile):
                step(t, 0)
        else:
            lax.fori_loop(0, width // tile, step, 0)

    first_beside = min(early + 1, chunks)
    spread_beside(0)
    spread_rest(0, 0)
    for c in range(1, first_beside):
        spread_beside(c)
    for c in range(1, min(2, early)):
        spread_rest(c, 0)
    for i, (c, h) in enumerate(steps):
        relay(c, h)
        compute(c, h)
        cross(c, h)
        if i == 0:
            for late in range(first_beside, chunks):
                spread_beside(late)
            for late in range(2, early):
                spread_rest(late, 0)
        else:
            finish(*steps[i - 1])
        for unit in spreads[i]:
            spread_rest(*unit)

    def slots_of(lo, hi):
        return [(c * block, (c + 1) * block) for c in range(lo, hi)]

    last = chunks - 1
    for c in range(early, chunks):
        cross_own(c)
    for c in range(early):
        arrived(c, 0)
        arrived(c, 1)
    pick(slots_of(0, early), False, False)
    finish(*steps[-1])

    def others_of(lo, hi):
        return [(c * block + ROWS, (c + 1) * block) for c in range(lo, hi)]

    for c in range(early, last - 1):
        arrived(c, 0)
        arrived(c, 1)
    pick(others_of(early, last - 1), True, False)
    arrived(last - 1, 0)
    arrived(last - 1, 1)
    pick(others_of(last - 1, last), True, False)

    every = rows.at[:, 0]
    but_own = pl.ds(ROWS, block - ROWS)
    copy_to(packed.at[:, but_own], rows.at[:, 0, but_own], go_sem, go_sem, core).wait_send()
    for kind in range(3):
        copy_to(every, every, pair_go.at[kind], go_sem, core).wait_send()
        copy_to(every, every, part_go.at[kind], go_sem, core).wait_send()
    copy_to(part.at[:, 0, but_own], rows.at[:, 0, but_own], ret_go, go_sem, core).wait_send()
    arrived(last, 0)
    arrived(last, 1)
    for c in range(early, chunks):
        finish_own(c)
    own_slots = [(c * block, c * block + ROWS) for c in range(early, last)]
    pick(own_slots + slots_of(last, chunks), True, True)


def plan(chunks):
    early = chunks // 2
    steps = [(c, 0) for c in range(early - 1)]
    steps += [(c, 1) for c in range(early - 1)] + [(early - 1, 0)]
    steps += [(c, 1) for c in range(early - 1, chunks)]
    steps += [(c, 0) for c in range(early, chunks)]
    waiting = [(c, h) for c, h in steps if h == 1 or c >= early]
    ahead = []
    done = 0
    for i in range(len(steps)):
        later = [u for u in steps[i + 1 :] if u in waiting]
        depth = 1 if i in (0, early - 1, early) else 2
        if steps[i] in [(chunks - 2, 1), (chunks - 1, 1)]:
            depth = 3
        wanted = later[:depth]
        upto = max([done] + [waiting.index(u) + 1 for u in wanted])
        ahead.append(waiting[done:upto])
        done = upto
    return early, steps, ahead


def expert_layer(ids, table, tokens, w_in, w_out, n, slots):
    exp_local, width, quarter = w_in.shape
    tok = tokens.shape[0]
    chunks = exp_local * slots // ROWS
    block = n * ROWS
    bf16 = jnp.bfloat16
    dma = pltpu.SemaphoreType.DMA
    anywhere = pl.BlockSpec(memory_space=pl.ANY)
    return pl.pallas_call(
        functools.partial(layer_kernel, n, slots),
        out_shape=pltpu.VMEM(tokens.shape, bf16),
        in_specs=[anywhere] * 5,
        out_specs=pl.BlockSpec(memory_space=pltpu.VMEM),
        scratch_shapes=[
            pltpu.VMEM(ids.shape, jnp.int32),
            pltpu.VMEM(table.shape, jnp.int32),
            pltpu.VMEM(tokens.shape, bf16),
            pltpu.VMEM((chunks, block, width), bf16),
            pltpu.VMEM((chunks * block, width), bf16),
            pltpu.VMEM((tok, LANES), jnp.int32),
            pltpu.VMEM(tokens.shape, bf16),
            pltpu.VMEM(w_in.shape, bf16),
            pltpu.VMEM(w_out.shape, bf16),
            pltpu.VMEM((chunks, 4, block, width), bf16),
            pltpu.VMEM((2 * block, quarter), bf16),
            pltpu.VMEM((chunks, 4, block, width), bf16),
            pltpu.VMEM((chunks, 2, block, width), bf16),
            pltpu.VMEM((chunks, block, width), bf16),
            dma((5,)),
            dma,
            dma((chunks, 3)),
            dma((3,)),
            dma((3, chunks, 2)),
            dma((3,)),
            dma((2, chunks, 2)),
            dma((chunks, 4)),
            dma,
            dma((chunks, 2)),
        ],
        compiler_params=pltpu.CompilerParams(
            collective_id=0, has_side_effects=True, vmem_limit_bytes=60 * 1024 * 1024
        ),
    )(ids, table, tokens, w_in, w_out)


def plain(tokens, token_ids, table, w_in, w_out):
    groups = lax.axis_size("expert")
    exp_local = w_in.shape[0]
    experts = groups * exp_local
    tok_rows, width = tokens.shape
    slots = max(2, 2 * tok_rows // experts)
    quarter = w_out.shape[1]
    chosen = jnp.take(table, token_ids, axis=0)
    expert_hot = (chosen[:, None] == jnp.arange(experts, dtype=jnp.int32)[None, :]).astype(
        jnp.int32
    )
    earlier = jnp.cumsum(expert_hot, axis=0) - expert_hot
    rank_tok = jnp.sum(earlier * expert_hot, axis=1)
    kept = rank_tok < slots
    column = (chosen // exp_local * slots + rank_tok) * exp_local + chosen % exp_local
    placer = (
        (column[:, None] == jnp.arange(experts * slots, dtype=jnp.int32)[None, :]) & kept[:, None]
    ).astype(jnp.bfloat16)
    packed = jnp.einsum("ts,td->sd", placer, tokens, preferred_element_type=jnp.float32).astype(
        jnp.bfloat16
    )
    packed = packed.reshape(groups * slots, exp_local, width)
    arrived = lax.all_to_all(packed, "expert", split_axis=0, concat_axis=0, tiled=True)
    rows = arrived.shape[0]
    hidden = jax.nn.relu(
        jnp.einsum(
            "red,edh->reh",
            arrived,
            lax.all_gather(w_in, "pair", axis=2, tiled=True),
            preferred_element_type=jnp.float32,
        )
    ).astype(jnp.bfloat16)
    total = jnp.zeros((rows, exp_local, width), jnp.float32)
    piece = lax.all_gather(w_out, "pair", axis=1, tiled=True)
    for index in range(piece.shape[1] // quarter):
        cols = lax.dynamic_slice_in_dim(hidden, index * quarter, quarter, 2)
        part = jnp.einsum(
            "reh,ehd->red",
            cols,
            piece[:, index * quarter : (index + 1) * quarter],
            preferred_element_type=jnp.float32,
        ).astype(jnp.bfloat16)
        total = total + lax.optimization_barrier(part).astype(jnp.float32)
    result = total.astype(jnp.bfloat16)
    returned = lax.all_to_all(result, "expert", split_axis=0, concat_axis=0, tiled=True)
    flat = returned.reshape(experts * slots, width)
    return jnp.dot(placer, flat, preferred_element_type=jnp.float32).astype(jnp.bfloat16)


def on_device(tokens, token_ids, table, w_in, w_out):
    n = lax.axis_size("expert")
    exp_local = w_in.shape[0]
    experts = n * exp_local
    tok_rows, width = tokens.shape
    slots = max(2, 2 * tok_rows // experts)
    fits = slots % ROWS == 0 and tok_rows % LANES == 0 and table.shape[0] % LANES == 0
    fits = fits and lax.axis_size("pair") == 4 and experts <= 256 and n == LANES // ROWS
    fits = fits and width % (4 * TILE) == 0 and w_in.shape[2] % TILE == 0
    if not fits or exp_local * slots // ROWS < 4:
        return plain(tokens, token_ids, table, w_in, w_out)
    return expert_layer(
        token_ids, table.reshape(-1, LANES), tokens, w_in, w_out, n, slots
    )


def solution(mesh):
    in_specs = (
        P(("expert", "pair"), None),
        P(("expert", "pair")),
        P(),
        P("expert", None, "pair"),
        P("expert", "pair", None),
    )
    out_specs = P(("expert", "pair"), None)
    return jax.shard_map(
        on_device, mesh=mesh, in_specs=in_specs, out_specs=out_specs, check_vma=False
    )
```

```python
import functools

import jax
import jax.numpy as jnp
from jax import lax
from jax.experimental import pallas as pl
from jax.experimental.pallas import tpu as pltpu
from jax.sharding import PartitionSpec as P

ROWS = 16
TILE = 256
LANES = 128
MESH = pl.DeviceIdType.MESH


def exact_dot(a, b):
    return jnp.dot(a, b, preferred_element_type=jnp.float32)


def across(me, j):
    other = me
    bit = 1
    while bit <= j:
        if j & bit:
            other = other + bit * (1 - 2 * (me // bit % 2))
        bit *= 2
    return other


def places(shape, dim):
    return lax.broadcasted_iota(jnp.int32, shape, dim)


def one_hot(flags):
    return jnp.where(flags, 1.0, 0.0).astype(jnp.bfloat16)


def slot_of_token(ids, table, me, exp_local, n, slots, per_expert):
    tok = ids.shape[1]
    lines = table.astype(jnp.float32).astype(jnp.bfloat16)
    line = one_hot(places((lines.shape[0], tok), 0) == ids // LANES)
    found = lax.dot_general(
        lines, line, (((0,), (0,)), ((), ())), preferred_element_type=jnp.float32
    )
    lane = places((LANES, tok), 0) == ids % LANES
    chosen = jnp.sum(jnp.where(lane, found, 0.0), axis=0, keepdims=True).astype(jnp.int32)
    hot = places((exp_local * n, tok), 0) == chosen
    before = places((tok, tok), 0) < places((tok, tok), 1)
    earlier = exact_dot(one_hot(hot), one_hot(before))
    rank = jnp.sum(jnp.where(hot, earlier, 0.0), axis=0, keepdims=True).astype(jnp.int32)
    group = chosen // exp_local
    ahead = jnp.bitwise_xor(group, me)
    chunk = chosen % exp_local * per_expert + rank // ROWS
    return jnp.where(rank < slots, (chunk * n + ahead) * ROWS + rank % ROWS, -1)


def layer_kernel(
    n,
    slots,
    ids_in,
    table_in,
    tokens_in,
    w_in,
    w_out,
    result,
    ids,
    table,
    tokens,
    packed,
    back,
    column,
    mixed,
    first,
    second,
    rows,
    hidden,
    part,
    near,
    far,
    in_sem,
    go_sem,
    come_sem,
    pair_go,
    pair_come,
    part_go,
    part_come,
    far_come,
    ret_go,
    ret_come,
):
    chunks, block, width = packed.shape
    exp_local = w_in.shape[0]
    per_expert = chunks // exp_local
    half = n // 2
    me = lax.axis_index("expert")
    at = lax.axis_index("pair")
    core = {"pair": at + 1 - 2 * (at % 2)}
    chip = {"pair": (at + 2) % 4}
    ahead = [{"expert": across(me, j)} for j in range(n)]

    loads = [
        pltpu.make_async_copy(src, dst, in_sem.at[k])
        for k, (src, dst) in enumerate(
            [(ids_in, ids), (table_in, table), (tokens_in, tokens), (w_in, first), (w_out, second)]
        )
    ]
    barrier = pltpu.get_barrier_semaphore()
    for peer in [core, chip] + ahead[1:]:
        pl.semaphore_signal(barrier, inc=1, device_id=peer, device_id_type=MESH)
    for copy in loads:
        copy.start()

    loads[0].wait()
    loads[1].wait()
    slot = slot_of_token(ids[...].reshape(1, ids.shape[0]), table[...], me, exp_local, n, slots, per_expert)
    tok = slot.shape[1]
    column[...] = jnp.transpose(jnp.broadcast_to(slot, (LANES, tok)))
    loads[2].wait()

    def copy_to(src, dst, send, recv, peer):
        return pltpu.make_async_remote_copy(
            src_ref=src,
            dst_ref=dst,
            send_sem=send,
            recv_sem=recv,
            device_id=peer,
            device_id_type=MESH,
        )

    def blocks(lo, hi):
        return pl.ds(lo * ROWS, (hi - lo) * ROWS)

    def span(c, lo, hi):
        return pl.ds(c * block + lo * ROWS, (hi - lo) * ROWS)

    own = blocks(0, 1)
    groups = [(1, 2), (2, half), (half, n)]
    group_of = [g for j in range(n) for g in range(3) if groups[g][0] <= max(j, 1) < groups[g][1]]
    bounds = [(0, half), (half, n)]

    def send_block(c, j):
        some = blocks(j, j + 1)
        recv = come_sem.at[c, group_of[j]]
        copy_to(packed.at[c, some], rows.at[c, 0, some], go_sem, recv, ahead[j]).start()

    def wait_blocks(c, g):
        some = blocks(*groups[g])
        copy_to(
            packed.at[c, some], rows.at[c, 0, some], go_sem, come_sem.at[c, g], ahead[1]
        ).wait_recv()

    def to_pair(kind, c, h, some, start):
        if kind == 0:
            src, dst, peer = rows.at[c, 0, some], rows.at[c, 2, some], chip
        elif kind == 1:
            src, dst, peer = rows.at[c, 0, some], rows.at[c, 1, some], core
        else:
            src, dst, peer = rows.at[c, 2, some], rows.at[c, 3, some], core
        copy = copy_to(src, dst, pair_go.at[kind], pair_come.at[min(kind, 1), c, h], peer)
        if start:
            copy.start()
        else:
            copy.wait_recv()

    def spread(c, h, lo, hi):
        to_pair(0, c, h, blocks(lo, hi), True)
        to_pair(1, c, h, blocks(lo, hi), True)

    def pack(c):
        placer = one_hot(places((block, tok), 0) + c * block == slot)
        wide_tile = 4 * TILE

        def step(t, carry):
            cols = pl.ds(pl.multiple_of(t * wide_tile, wide_tile), wide_tile)
            x = exact_dot(placer, tokens[:, cols]).astype(jnp.bfloat16)
            packed[c, :, cols] = x
            rows[c, 0, own, cols] = x[:ROWS]
            return carry

        lax.fori_loop(0, width // wide_tile, step, 0)

    early, steps, spreads = plan(chunks)

    def dispatch(c, h):
        for j in range(*groups[1 + h]):
            send_block(c, j)

    pack(0)
    pack(1)
    pl.semaphore_wait(barrier, n + 1)
    for c in range(chunks):
        if c > 1:
            pack(c)
        spread(c, 0, 0, 1)
        send_block(c, 1)
        dispatch(c, 0)
        if c == 0:
            dispatch(0, 1)
    for c in range(1, chunks):
        dispatch(c, 1)
    def spread_rest(c, h):
        wait_blocks(c, 1 + h)
        spread(c, h, *groups[1 + h])

    def spread_beside(c):
        wait_blocks(c, 0)
        spread(c, 0, 1, 2)

    def relay(c, h):
        to_pair(0, c, h, blocks(*bounds[h]), False)
        to_pair(2, c, h, blocks(*bounds[h]), True)

    def to_part(kind, c, p, some, start):
        if kind == 0:
            src, dst, peer = part.at[c, 3, some], near.at[c, 1, some], core
        elif kind == 1:
            src, dst, peer = part.at[c, 1, some], near.at[c, 0, some], core
        else:
            src, dst, peer = part.at[c, 2, some], far.at[c, some], chip
        recv = far_come.at[c, p] if kind == 2 else part_come.at[kind, c, p]
        copy = copy_to(src, dst, part_go.at[kind], recv, peer)
        if start:
            copy.start()
        else:
            copy.wait_recv()

    def compute(c, h):
        e = c // per_expert
        if (c, h) == steps[0]:
            for copy in loads[3:]:
                copy.wait()
        some = blocks(*bounds[h])
        size = (bounds[h][1] - bounds[h][0]) * ROWS
        both = rows.at[c, pl.ds(0, 2), some]
        copy_to(both, both, pair_go.at[1], pair_come.at[1, c, h], core).wait_recv()

        def project_in(t, carry):
            cols = pl.ds(pl.multiple_of(t * TILE, TILE), TILE)
            x = rows[c, :, some].reshape(4 * size, width)
            hid = exact_dot(x, first[e, :, cols])
            hidden[:, cols] = jnp.maximum(hid, 0.0).astype(jnp.bfloat16)
            return carry

        lax.fori_loop(0, first.shape[2] // TILE, project_in, 0, unroll=True)

        def project_out(t, carry):
            tile = 2 * TILE
            cols = pl.ds(pl.multiple_of(t * tile, tile), tile)
            y = exact_dot(hidden[...], second[e, :, cols]).astype(jnp.bfloat16)
            for k in range(4):
                part[c, k, some, cols] = y[k * size : (k + 1) * size]
            return carry

        lax.fori_loop(0, width // (2 * TILE), project_out, 0, unroll=2)
        to_part(0, c, h, some, True)
        to_part(1, c, h, some, True)

    def over_rows(lo, hi, body):
        def step(t, carry):
            body(pl.ds(pl.multiple_of(t * ROWS, ROWS), ROWS))
            return carry

        lax.fori_loop(lo, hi, step, 0)

    def wide(x):
        return x.astype(jnp.float32)

    def pieces(c, h):
        if h == 0 and c >= early:
            return [(2, half, 0), (1, 2, 2)]
        return [bounds[h] + (h,)]

    def cross(c, h):
        to_part(0, c, h, blocks(*bounds[h]), False)

        def add(r):
            both = wide(part[c, 2, r]) + wide(near[c, 1, r])
            part[c, 2, r] = both.astype(jnp.bfloat16)

        for lo, hi, p in pieces(c, h):
            over_rows(lo, hi, add)
            to_part(2, c, p, blocks(lo, hi), True)

    def cross_own(c):
        both = wide(part[c, 2, own]) + wide(near[c, 1, own])
        part[c, 2, own] = both.astype(jnp.bfloat16)
        to_part(2, c, 3, own, True)

    def sum_up(c, r):
        both = wide(part[c, 0, r]) + wide(near[c, 0, r])
        return (both + wide(far[c, r])).astype(jnp.bfloat16)

    def finish_own(c):
        to_part(2, c, 3, own, False)
        back[span(c, 0, 1)] = sum_up(c, own)

    def finish(c, h):
        to_part(1, c, h, blocks(*bounds[h]), False)
        for lo, hi, p in pieces(c, h):
            to_part(2, c, p, blocks(lo, hi), False)

            def add(r):
                part[c, 0, r] = sum_up(c, r)

            over_rows(lo, hi, add)
            for j in range(max(lo, 1), hi):
                copy_to(
                    part.at[c, 0, blocks(j, j + 1)],
                    back.at[span(c, j, j + 1)],
                    ret_go,
                    ret_come.at[c, h],
                    ahead[j],
                ).start()
            if lo == 0:
                back[span(c, 0, 1)] = part[c, 0, own]

    def arrived(c, h):
        lo, hi = bounds[h]
        lo = max(lo, 1)
        copy_to(
            part.at[c, 0, blocks(lo, hi)],
            back.at[span(c, lo, hi)],
            ret_go,
            ret_come.at[c, h],
            ahead[1],
        ).wait_recv()

    def pick(ranges, more, store):
        picker = jnp.concatenate(
            [
                one_hot(column[:, : hi - lo] == places((tok, hi - lo), 1) + lo)
                for lo, hi in ranges
            ],
            axis=1,
        )

        tile = (2 if store else 4) * TILE

        def step(t, carry):
            some = pl.ds(pl.multiple_of(t * tile, tile), tile)
            x = jnp.concatenate([back[lo:hi, some] for lo, hi in ranges], axis=0)
            y = exact_dot(picker, x)
            if more:
                y = y + wide(mixed[:, some])
            (result if store else mixed)[:, some] = y.astype(jnp.bfloat16)
            return carry

        if store:
            for t in range(width // tile):
                step(t, 0)
        else:
            lax.fori_loop(0, width // tile, step, 0)

    first_beside = min(early + 1, chunks)
    spread_beside(0)
    spread_rest(0, 0)
    for c in range(1, first_beside):
        spread_beside(c)
    for c in range(1, min(2, early)):
        spread_rest(c, 0)
    for i, (c, h) in enumerate(steps):
        relay(c, h)
        compute(c, h)
        cross(c, h)
        if i == 0:
            for late in range(first_beside, chunks):
                spread_beside(late)
            for late in range(2, early):
                spread_rest(late, 0)
        else:
            finish(*steps[i - 1])
        for unit in spreads[i]:
            spread_rest(*unit)

    def slots_of(lo, hi):
        return [(c * block, (c + 1) * block) for c in range(lo, hi)]

    last = chunks - 1
    for c in range(early, chunks):
        cross_own(c)
    for c in range(early):
        arrived(c, 0)
        arrived(c, 1)
    pick(slots_of(0, early), False, False)
    finish(*steps[-1])

    def others_of(lo, hi):
        return [(c * block + ROWS, (c + 1) * block) for c in range(lo, hi)]

    for c in range(early, last - 1):
        arrived(c, 0)
        arrived(c, 1)
    pick(others_of(early, last - 1), True, False)
    arrived(last - 1, 0)
    arrived(last - 1, 1)
    pick(others_of(last - 1, last), True, False)

    every = rows.at[:, 0]
    but_own = pl.ds(ROWS, block - ROWS)
    copy_to(packed.at[:, but_own], rows.at[:, 0, but_own], go_sem, go_sem, core).wait_send()
    for kind in range(3):
        copy_to(every, every, pair_go.at[kind], go_sem, core).wait_send()
        copy_to(every, every, part_go.at[kind], go_sem, core).wait_send()
    copy_to(part.at[:, 0, but_own], rows.at[:, 0, but_own], ret_go, go_sem, core).wait_send()
    arrived(last, 0)
    arrived(last, 1)
    for c in range(early, chunks):
        finish_own(c)
    own_slots = [(c * block, c * block + ROWS) for c in range(early, last)]
    pick(own_slots + slots_of(last, chunks), True, True)


def plan(chunks):
    early = chunks // 2
    steps = [(c, 0) for c in range(early - 1)]
    steps += [(c, 1) for c in range(early - 1)] + [(early - 1, 0)]
    steps += [(c, 1) for c in range(early - 1, chunks)]
    steps += [(c, 0) for c in range(early, chunks)]
    waiting = [(c, h) for c, h in steps if h == 1 or c >= early]
    ahead = []
    done = 0
    for i in range(len(steps)):
        later = [u for u in steps[i + 1 :] if u in waiting]
        depth = 1 if i in (0, early - 1, early) else 2
        if steps[i] in [(chunks - 2, 1), (chunks - 1, 1)]:
            depth = 3
        wanted = later[:depth]
        upto = max([done] + [waiting.index(u) + 1 for u in wanted])
        ahead.append(waiting[done:upto])
        done = upto
    return early, steps, ahead


def expert_layer(ids, table, tokens, w_in, w_out, n, slots):
    exp_local, width, quarter = w_in.shape
    tok = tokens.shape[0]
    chunks = exp_local * slots // ROWS
    block = n * ROWS
    bf16 = jnp.bfloat16
    dma = pltpu.SemaphoreType.DMA
    anywhere = pl.BlockSpec(memory_space=pl.ANY)
    return pl.pallas_call(
        functools.partial(layer_kernel, n, slots),
        out_shape=pltpu.VMEM(tokens.shape, bf16),
        in_specs=[anywhere] * 5,
        out_specs=pl.BlockSpec(memory_space=pltpu.VMEM),
        scratch_shapes=[
            pltpu.VMEM(ids.shape, jnp.int32),
            pltpu.VMEM(table.shape, jnp.int32),
            pltpu.VMEM(tokens.shape, bf16),
            pltpu.VMEM((chunks, block, width), bf16),
            pltpu.VMEM((chunks * block, width), bf16),
            pltpu.VMEM((tok, LANES), jnp.int32),
            pltpu.VMEM(tokens.shape, bf16),
            pltpu.VMEM(w_in.shape, bf16),
            pltpu.VMEM(w_out.shape, bf16),
            pltpu.VMEM((chunks, 4, block, width), bf16),
            pltpu.VMEM((2 * block, quarter), bf16),
            pltpu.VMEM((chunks, 4, block, width), bf16),
            pltpu.VMEM((chunks, 2, block, width), bf16),
            pltpu.VMEM((chunks, block, width), bf16),
            dma((5,)),
            dma,
            dma((chunks, 3)),
            dma((3,)),
            dma((2, chunks, 2)),
            dma((3,)),
            dma((2, chunks, 2)),
            dma((chunks, 4)),
            dma,
            dma((chunks, 2)),
        ],
        compiler_params=pltpu.CompilerParams(
            collective_id=0, has_side_effects=True, vmem_limit_bytes=60 * 1024 * 1024
        ),
    )(ids, table, tokens, w_in, w_out)


def plain(tokens, token_ids, table, w_in, w_out):
    groups = lax.axis_size("expert")
    exp_local = w_in.shape[0]
    experts = groups * exp_local
    tok_rows, width = tokens.shape
    slots = max(2, 2 * tok_rows // experts)
    quarter = w_out.shape[1]
    chosen = jnp.take(table, token_ids, axis=0)
    expert_hot = (chosen[:, None] == jnp.arange(experts, dtype=jnp.int32)[None, :]).astype(
        jnp.int32
    )
    earlier = jnp.cumsum(expert_hot, axis=0) - expert_hot
    rank_tok = jnp.sum(earlier * expert_hot, axis=1)
    kept = rank_tok < slots
    column = (chosen // exp_local * slots + rank_tok) * exp_local + chosen % exp_local
    placer = (
        (column[:, None] == jnp.arange(experts * slots, dtype=jnp.int32)[None, :]) & kept[:, None]
    ).astype(jnp.bfloat16)
    packed = jnp.einsum("ts,td->sd", placer, tokens, preferred_element_type=jnp.float32).astype(
        jnp.bfloat16
    )
    packed = packed.reshape(groups * slots, exp_local, width)
    arrived = lax.all_to_all(packed, "expert", split_axis=0, concat_axis=0, tiled=True)
    rows = arrived.shape[0]
    hidden = jax.nn.relu(
        jnp.einsum(
            "red,edh->reh",
            arrived,
            lax.all_gather(w_in, "pair", axis=2, tiled=True),
            preferred_element_type=jnp.float32,
        )
    ).astype(jnp.bfloat16)
    total = jnp.zeros((rows, exp_local, width), jnp.float32)
    piece = lax.all_gather(w_out, "pair", axis=1, tiled=True)
    for index in range(piece.shape[1] // quarter):
        cols = lax.dynamic_slice_in_dim(hidden, index * quarter, quarter, 2)
        part = jnp.einsum(
            "reh,ehd->red",
            cols,
            piece[:, index * quarter : (index + 1) * quarter],
            preferred_element_type=jnp.float32,
        ).astype(jnp.bfloat16)
        total = total + lax.optimization_barrier(part).astype(jnp.float32)
    result = total.astype(jnp.bfloat16)
    returned = lax.all_to_all(result, "expert", split_axis=0, concat_axis=0, tiled=True)
    flat = returned.reshape(experts * slots, width)
    return jnp.dot(placer, flat, preferred_element_type=jnp.float32).astype(jnp.bfloat16)


def on_device(tokens, token_ids, table, w_in, w_out):
    n = lax.axis_size("expert")
    exp_local = w_in.shape[0]
    experts = n * exp_local
    tok_rows, width = tokens.shape
    slots = max(2, 2 * tok_rows // experts)
    fits = slots % ROWS == 0 and tok_rows % LANES == 0 and table.shape[0] % LANES == 0
    fits = fits and lax.axis_size("pair") == 4 and experts <= 256 and n == LANES // ROWS
    fits = fits and width % (4 * TILE) == 0 and w_in.shape[2] % TILE == 0
    if not fits or exp_local * slots // ROWS < 4:
        return plain(tokens, token_ids, table, w_in, w_out)
    return expert_layer(
        token_ids, table.reshape(-1, LANES), tokens, w_in, w_out, n, slots
    )


def solution(mesh):
    in_specs = (
        P(("expert", "pair"), None),
        P(("expert", "pair")),
        P(),
        P("expert", None, "pair"),
        P("expert", "pair", None),
    )
    out_specs = P(("expert", "pair"), None)
    return jax.shard_map(
        on_device, mesh=mesh, in_specs=in_specs, out_specs=out_specs, check_vma=False
    )
```
